512 devices in a mesh: tm: 128 (over z, x, y_hi), chan: 4 (over y_lo, core).
Axes of the slice: x: 4, y: 4 (y_hi: 2, y_lo: 2; y = y_hi * 2 + y_lo), z: 16, core: 2. Of those that a mesh axis runs over, the one named last changes fastest.
Arguments:
- frames: bfloat16 [65536, 1024], P('tm', 'chan'), may hold values from -6 to 6
- w_in: bfloat16 [3, 1024, 1024], P(None, None, 'chan'), may hold values from -0.1875 to 0.1875
- short_taps: float32 [3, 3, 1024], P(None, None, 'chan'), may hold values from -3 to 3
- filter_taps: bfloat16 [65536, 1024], P('tm', 'chan'), may hold values from -0.0234375 to 0.0234375
- skip_gain: float32 [1024], P('chan'), may hold values from -4 to 4
- w_out: bfloat16 [1024, 1024], P(None, 'chan'), may hold values from -0.1875 to 0.1875
Outputs:
- layer_out: bfloat16 [65536, 1024], P('tm', 'chan')
The draws below stay inside these ranges and needn't reach their ends.
All inputs are finite; a program needn't handle non-finite values.
Results may differ from the reference program's by a relative error of at most 0.011.
Values may be sent and summed in bfloat16 or wider, within the bound.
A program may use at most 64 MiB of HBM per device.

```python
import jax
import jax.numpy as jnp
from jax import lax

D = 1024
TOK_DEV = 512
SEQ = 65536
N_TM = 128
N_CHAN = 4


def levels(own_key, shape, cuts, least, largest):
    def one(axis_at, shards_of):
        steps = jax.random.uniform(jax.random.fold_in(jax.random.fold_in(own_key, 6), axis_at), (shards_of,), jnp.float32, least / len(cuts), largest / len(cuts))
        return jnp.repeat(jnp.exp(steps), shape[axis_at] // shards_of).reshape((-1,) + (1,) * (len(shape) - axis_at - 1))

    loudness = one(*cuts[0])
    for cut in cuts[1:]:
        loudness = loudness * one(*cut)
    return loudness


def centred(own_key, dims, deviation, bound, split=(), kind=jnp.bfloat16):
    entries = jax.random.normal(own_key, dims, jnp.float32) * deviation
    if len(split) > 0:
        entries = levels(own_key, dims, split, -0.22, 0.18) * entries
    return jnp.clip(entries, min=-bound, max=bound).astype(kind)


def setup_inputs(seed: int = 0) -> dict:
    key_list = jax.random.split(jax.random.key(seed), 7)
    frames = centred(key_list[0], (SEQ, D), 1.0, 6.0, ((0, 128), (1, 4)))
    w_in = centred(key_list[1], (3, D, D), D ** -0.5, 0.1875, ((2, 4),))
    short_taps = centred(key_list[2], (3, 3, D), 0.6, 3.0, ((2, 4),), jnp.float32)
    filter_taps = centred(key_list[3], (SEQ, D), SEQ ** -0.5, 0.0234375, ((0, 128), (1, 4)))
    skip_gain = centred(key_list[4], (D,), 1.0, 4.0, ((0, 4),), jnp.float32)
    w_out = centred(key_list[5], (D, D), D ** -0.5, 0.1875, ((1, 4),))
    return {"frames": frames, "w_in": w_in, "short_taps": short_taps, "filter_taps": filter_taps, "skip_gain": skip_gain, "w_out": w_out}


def angle_table(first, second, modulus):
    index = (first[:, None] * second[None, :]) % modulus
    return (2.0 * jnp.pi / modulus) * index.astype(jnp.float32)


def contract(form, left, right):
    return jnp.einsum(form, left.astype(jnp.float32), right.astype(jnp.float32))


def column_section(block, row_cos, row_sin, turn_cos, turn_sin):
    real_part = contract("rcd,rk->kcd", block, row_cos)
    imag_part = -contract("rcd,rk->kcd", block, row_sin)
    cosine = turn_cos[:, :, None]
    sine = turn_sin[:, :, None]
    turned_real = real_part * cosine + imag_part * sine
    turned_imag = imag_part * cosine - real_part * sine
    return jnp.stack([turned_real, turned_imag]).astype(jnp.bfloat16)


def spectrum_section(parts, col_cos, col_sin):
    real_part = contract("kcd,cm->kmd", parts[0], col_cos) + contract("kcd,cm->kmd", parts[1], col_sin)
    imag_part = contract("kcd,cm->kmd", parts[1], col_cos) - contract("kcd,cm->kmd", parts[0], col_sin)
    return real_part, imag_part


def product_section(first, second, points):
    real_part = (first[0] * second[0] - first[1] * second[1]) / points
    imag_part = (first[0] * second[1] + first[1] * second[0]) / points
    return jnp.stack([real_part, imag_part]).astype(jnp.bfloat16)


def inverse_section(parts, col_cos, col_sin, turn_cos, turn_sin):
    real_part = contract("kmd,cm->kcd", parts[0], col_cos) - contract("kmd,cm->kcd", parts[1], col_sin)
    imag_part = contract("kmd,cm->kcd", parts[0], col_sin) + contract("kmd,cm->kcd", parts[1], col_cos)
    cosine = turn_cos[:, :, None]
    sine = turn_sin[:, :, None]
    turned_real = real_part * cosine - imag_part * sine
    turned_imag = real_part * sine + imag_part * cosine
    return jnp.stack([turned_real, turned_imag]).astype(jnp.bfloat16)


def row_section(parts, row_cos, row_sin):
    result = contract("kcd,rk->rcd", parts[0], row_cos) - contract("kcd,rk->rcd", parts[1], row_sin)
    return result.astype(jnp.bfloat16)


def reference(frames, w_in, short_taps, filter_taps, skip_gain, w_out):
    width = frames.shape[1]
    projected = contract("td,jde->jte", frames, w_in).astype(jnp.bfloat16)
    padded = jnp.pad(projected.astype(jnp.float32), ((0, 0), (2, 0), (0, 0)))
    shorted = (short_taps[:, 0][:, None, :] * padded[:, 2:]
               + short_taps[:, 1][:, None, :] * padded[:, 1:-1]
               + short_taps[:, 2][:, None, :] * padded[:, :-2])
    query, key, value = shorted[0], shorted[1], shorted[2]
    signal = (key * value).astype(jnp.bfloat16)
    freq_rows = 2 * N_TM
    points = freq_rows * TOK_DEV
    row_index = jnp.arange(N_TM, dtype=jnp.int32)
    freq_index = jnp.arange(freq_rows, dtype=jnp.int32)
    col_index = jnp.arange(TOK_DEV, dtype=jnp.int32)
    row_angle = angle_table(row_index, freq_index, freq_rows)
    col_angle = angle_table(col_index, col_index, TOK_DEV)
    row_cos = jnp.cos(row_angle).astype(jnp.bfloat16)
    row_sin = jnp.sin(row_angle).astype(jnp.bfloat16)
    col_cos = jnp.cos(col_angle).astype(jnp.bfloat16)
    col_sin = jnp.sin(col_angle).astype(jnp.bfloat16)
    turn_angle = angle_table(freq_index, col_index, points)
    turn_cos = jnp.cos(turn_angle)
    turn_sin = jnp.sin(turn_angle)
    group_size = width // N_CHAN
    groups = width // group_size
    signal_groups = signal.reshape(N_TM, TOK_DEV, groups, group_size).transpose(2, 0, 1, 3)
    filter_groups = filter_taps.reshape(N_TM, TOK_DEV, groups, group_size).transpose(2, 0, 1, 3)

    def convolve(pair):
        signal_block, filter_block = pair
        column_signal = column_section(signal_block, row_cos, row_sin, turn_cos, turn_sin)
        column_filter = column_section(filter_block, row_cos, row_sin, turn_cos, turn_sin)
        spectrum_signal = spectrum_section(column_signal, col_cos, col_sin)
        spectrum_filter = spectrum_section(column_filter, col_cos, col_sin)
        response = product_section(spectrum_signal, spectrum_filter, points)
        back = inverse_section(response, col_cos, col_sin, turn_cos, turn_sin)
        return row_section(back, row_cos, row_sin)

    conv = lax.map(convolve, (signal_groups, filter_groups))
    conv = conv.transpose(1, 2, 0, 3).reshape(N_TM * TOK_DEV, width)
    gated = (query * (conv.astype(jnp.float32) + skip_gain * signal.astype(jnp.float32))).astype(jnp.bfloat16)
    mixing_sum = jnp.dot(gated, w_out, preferred_element_type=jnp.float32)
    return (mixing_sum + frames.astype(jnp.float32)).astype(jnp.bfloat16)
```

```python
import functools

import jax
import jax.numpy as jnp
import numpy as np
from jax import lax
from jax.experimental import pallas as pl
from jax.experimental.pallas import tpu as pltpu
from jax.sharding import PartitionSpec as P

MESH = pl.DeviceIdType.MESH
ROWS = 128
COLS = 512
CHANS = 256
PEERS = ROWS - 1
LANES = 128
F32 = jnp.float32
BF16 = jnp.bfloat16


def tables():
    r = np.arange(ROWS, dtype=np.int64)
    k = np.arange(ROWS, dtype=np.int64)
    c = np.arange(COLS, dtype=np.int64)
    row = (2.0 * np.pi / (4 * ROWS)) * ((r[None, :] * (4 * k[:, None] + 1)) % (4 * ROWS))
    turn = (2.0 * np.pi / (4 * ROWS * COLS)) * (c[None, :] * (4 * k[:, None] + 1))
    col = (2.0 * np.pi / COLS) * ((c[:, None] * c[None, :]) % COLS)
    row_both = np.concatenate([np.cos(row), -np.sin(row)], axis=0)
    return (
        jnp.asarray(row_both, BF16),
        jnp.asarray(row_both.T, BF16),
        jnp.asarray(np.cos(turn), F32),
        jnp.asarray(np.sin(turn), F32),
        jnp.asarray(np.cos(col), BF16),
        jnp.asarray(np.sin(col), BF16),
    )


def dot(left, right):
    return jnp.dot(left, right, preferred_element_type=F32)


def kernel(
    frames, filt, taps, skip, w_in_h, w_out_h, row_h, rowi_h, tc_h, ts_h, cc_h, cs_h,
    out,
    w_in, w_out, row, rowi, tcos, tsin, ccos, csin,
    xg, p, qf, sf, slab, fsend, frecv, ssend, srecv, csend, crecv, hsend, hrecv,
    gbuf, gg, gmat, q2, spec, xm, ym, bstack,
    load_sem, ag_s, ag_r, agf_s, agf_r, sib_s, sib_r,
    g_s, g_r, gf_s, gf_r, gs_s, gs_r, a_s, a_r, h_s, h_r,
):
    t = lax.axis_index("tm")
    q = lax.axis_index("chan")
    cross = lax.rem(q + 2, 4)
    sib = q + 1 - 2 * lax.rem(q, 2)

    barrier = pltpu.get_barrier_semaphore()

    def greet(d, carry):
        pl.semaphore_signal(
            barrier, 1, device_id={"tm": lax.rem(t + d, ROWS)}, device_id_type=MESH
        )
        return carry

    lax.fori_loop(1, ROWS, greet, 0)
    for peer in (cross, sib):
        pl.semaphore_signal(barrier, 1, device_id={"chan": peer}, device_id_type=MESH)

    loads = []
    pairs = (
        (w_in_h, w_in), (row_h, row), (tc_h, tcos), (ts_h, tsin), (cc_h, ccos),
        (cs_h, csin), (rowi_h, rowi), (w_out_h, w_out),
    )
    for i, (src, dst) in enumerate(pairs):
        copy = pltpu.make_async_copy(src, dst, load_sem.at[i])
        copy.start()
        loads.append(copy)

    def to_slabs(block_of, halves):
        for cb in halves:
            for e in range(2):
                slab[pl.ds(2 * cb + e, ROWS, stride=8), :] = jnp.transpose(block_of(cb, e))

    def pack(send):
        def step(i, carry):
            rows = slab[pl.ds(pl.multiple_of(i * LANES, LANES), LANES), :]
            send[pl.ds(i * 16, 16)] = rows.reshape(16, 8, LANES).astype(BF16)
            return carry

        lax.fori_loop(0, 8, step, 0)

    def unpack(recv):
        def step(i, carry):
            rows = recv[pl.ds(i * 16, 16)].astype(F32).reshape(LANES, LANES)
            slab[pl.ds(pl.multiple_of(i * LANES, LANES), LANES), :] = rows
            return carry

        lax.fori_loop(0, 8, step, 0)

    def offset(i):
        b = i // 8
        h = (b + 1) // 2
        zo = 8 + h - 2 * h * lax.rem(b, 2)
        return lax.rem(zo, 16) * 8 + 7 - lax.rem(i, 8)

    def spread(send, recv, which, rows):
        def step(i, carry):
            peer = lax.rem(t + offset(i), ROWS)
            pltpu.make_async_remote_copy(
                send.at[peer, rows], recv.at[t, rows], a_s.at[which], a_r.at[which],
                device_id={"tm": peer}, device_id_type=MESH,
            ).start()
            return carry

        lax.fori_loop(0, PEERS, step, 0)
        recv[t, rows] = send[t, rows]

    def await_recv(recv, which, rows):
        part = recv.at[pl.ds(0, PEERS), rows]
        pltpu.make_async_copy(part, part, a_r.at[which]).wait()

    def await_send(send, which, rows):
        part = send.at[pl.ds(0, PEERS), rows]
        pltpu.make_async_copy(part, part, a_s.at[which]).wait()

    ALL = pl.ds(0, 8)
    HALF = (pl.ds(0, 4), pl.ds(4, 4))

    to_slabs(
        lambda cb, e: filt[cb * 128 : cb * 128 + 128, e * 128 : e * 128 + 128].astype(F32),
        range(4),
    )
    pack(fsend)
    xg[q] = frames[...]
    pl.semaphore_wait(barrier, PEERS + 2)

    def gather_start(src, dst, i, s1, r1, s2, r2):
        rows = pl.ds(i * 256, 256)
        over = pltpu.make_async_remote_copy(
            src.at[rows], dst.at[q, rows], s1.at[i], r1.at[i],
            device_id={"chan": cross}, device_id_type=MESH,
        )
        over.start()
        near = pltpu.make_async_remote_copy(
            src.at[rows], dst.at[q, rows], s2.at[i], r2.at[i],
            device_id={"chan": sib}, device_id_type=MESH,
        )
        near.start()
        return over, near

    def gather_pass(dst, over, i, s3, r3):
        rows = pl.ds(i * 256, 256)
        over.wait_recv()
        on = pltpu.make_async_remote_copy(
            dst.at[cross, rows], dst.at[cross, rows], s3.at[i], r3.at[i],
            device_id={"chan": sib}, device_id_type=MESH,
        )
        on.start()
        return on

    order = (1, 0)
    first = {i: gather_start(frames, xg, i, ag_s, ag_r, sib_s, sib_r) for i in order}
    spread(fsend, frecv, 0, ALL)
    passed = {}
    loads[0].wait()

    def project(i):
        base = i * 256
        for j in range(3):
            total = dot(xg[0, base : base + 256], w_in[j, 0:256])
            for n in range(1, 4):
                total += dot(xg[n, base : base + 256], w_in[j, n * 256 : n * 256 + 256])
            p[16 + base : 16 + base + 256, j * 256 : j * 256 + 256] = total.astype(
                BF16
            ).astype(F32)

    for i in order:
        passed[i] = gather_pass(xg, first[i][0], i, agf_s, agf_r)
        first[i][1].wait_recv()
        passed[i].wait_recv()
        project(i)
        if i == 1:
            hsend[...] = p[512:528, :].astype(BF16)
            halo = pltpu.make_async_remote_copy(
                hsend, hrecv, h_s, h_r,
                device_id={"tm": lax.rem(t + 1, ROWS)}, device_id_type=MESH,
            )
            halo.start()

    def short(i):
        for base in range(i * 256, i * 256 + 256, 64):
            made = []
            for j in range(3):
                lanes = slice(j * 256, j * 256 + 256)
                made.append(
                    taps[j, 0:1, :] * p[16 + base : 80 + base, lanes]
                    + taps[j, 1:2, :] * p[15 + base : 79 + base, lanes]
                    + taps[j, 2:3, :] * p[14 + base : 78 + base, lanes]
                )
            qf[base : base + 64, :] = made[0]
            sf[base : base + 64, :] = (made[1] * made[2]).astype(BF16).astype(F32)

    block = lambda cb, e: sf[cb * 128 : cb * 128 + 128, e * 128 : e * 128 + 128]
    short(1)
    to_slabs(block, (2, 3))
    halo.wait_recv()
    p[0:16, :] = jnp.where(t > 0, hrecv[...].astype(F32), 0.0)
    short(0)
    to_slabs(block, (0, 1))
    pack(ssend)
    spread(ssend, srecv, 1, ALL)

    for copy in loads[1:]:
        copy.wait()

    def transform(recv):
        unpack(recv)
        for cb in range(4):
            for e in range(2):
                col = e * 512 + cb * 128
                gmat[:, col : col + 128] = slab[pl.ds(2 * cb + e, ROWS, stride=8), :].astype(BF16)
        for e in range(2):
            both = dot(row[...], gmat[:, e * 512 : e * 512 + 512])
            a, b = both[0:128], both[128:256]
            q2[e * 128 : e * 128 + 128, :] = (a * tcos[...] + b * tsin[...]).astype(BF16)
            q2[256 + e * 128 : 384 + e * 128, :] = (b * tcos[...] - a * tsin[...]).astype(BF16)
        xm[...] = dot(q2[...], ccos[...])
        ym[...] = dot(q2[...], csin[...])

    await_recv(frecv, 0, ALL)
    transform(frecv)
    spec[0:256, :] = xm[0:256, :] + ym[256:512, :]
    spec[256:512, :] = xm[256:512, :] - ym[0:256, :]

    await_recv(srecv, 1, ALL)
    transform(srecv)

    def multiply(i, carry):
        top = pl.ds(pl.multiple_of(i * 32, 32), 32)
        low = pl.ds(pl.multiple_of(256 + i * 32, 32), 32)
        sr = xm[top, :] + ym[low, :]
        si = xm[low, :] - ym[top, :]
        fr, fi = spec[top, :], spec[low, :]
        scale = 1.0 / (ROWS * COLS)
        q2[top, :] = ((sr * fr - si * fi) * scale).astype(BF16)
        q2[low, :] = ((sr * fi + si * fr) * scale).astype(BF16)
        return carry

    lax.fori_loop(0, 8, multiply, 0)

    for h in range(2):
        cols = slice(h * 256, h * 256 + 256)
        xm[:, cols] = dot(q2[...], ccos[:, cols])
        ym[:, cols] = dot(q2[...], csin[:, cols])
        for e in range(2):
            top = slice(e * 128, e * 128 + 128)
            low = slice(256 + e * 128, 384 + e * 128)
            br = xm[top, cols] - ym[low, cols]
            bi = ym[top, cols] + xm[low, cols]
            co, si = tcos[:, cols], tsin[:, cols]
            lanes = slice(e * 256, e * 256 + 256)
            bstack[0:128, lanes] = (br * co - bi * si).astype(BF16)
            bstack[128:256, lanes] = (br * si + bi * co).astype(BF16)
        conv = dot(rowi[...], bstack[...])
        for cb in range(2):
            for e in range(2):
                lane = e * 256 + cb * 128
                slab[pl.ds(4 * h + 2 * cb + e, ROWS, stride=8), :] = conv[:, lane : lane + 128]
        pack_half(slab, csend, h)
        spread(csend, crecv, 2 + h, HALF[h])

    second = {}
    onward = {}
    for h in range(2):
        await_recv(crecv, 2 + h, HALF[h])
        unpack_half(crecv, slab, h)
        for cb in range(2 * h, 2 * h + 2):
            for e in range(2):
                rows = slice(cb * 128, cb * 128 + 128)
                lanes = slice(e * 128, e * 128 + 128)
                conv = jnp.transpose(slab[pl.ds(2 * cb + e, ROWS, stride=8), :])
                gated = qf[rows, lanes] * (conv + skip[:, lanes] * sf[rows, lanes])
                gbuf[rows, lanes] = gated.astype(BF16)
        rows = slice(h * 256, h * 256 + 256)
        second[h] = gather_start(gbuf, gg, h, g_s, g_r, gs_s, gs_r)
        gg[q, rows] = gbuf[rows, :]

    for h in range(2):
        rows = slice(h * 256, h * 256 + 256)
        onward[h] = gather_pass(gg, second[h][0], h, gf_s, gf_r)
        second[h][1].wait_recv()
        onward[h].wait_recv()
        total = dot(gg[0, rows], w_out[0:256, :])
        for n in range(1, 4):
            total += dot(gg[n, rows], w_out[n * 256 : n * 256 + 256, :])
        out[rows, :] = (total + frames[rows, :].astype(F32)).astype(BF16)

    await_send(fsend, 0, ALL)
    await_send(ssend, 1, ALL)
    for h in range(2):
        await_send(csend, 2 + h, HALF[h])
    halo.wait_send()
    for group in (first, second):
        for over, near in group.values():
            over.wait_send()
            near.wait_send()
    for group in (passed, onward):
        for on in group.values():
            on.wait_send()


def pack_half(slab, send, h):
    def step(i, carry):
        rows = slab[pl.ds(pl.multiple_of(i * LANES, LANES), LANES), :].reshape(16, 8, LANES)
        send[pl.ds(i * 16, 16), 4 * h : 4 * h + 4] = rows[:, 4 * h : 4 * h + 4].astype(BF16)
        return carry

    lax.fori_loop(0, 8, step, 0)


def unpack_half(recv, slab, h):
    def step(i, carry):
        rows = recv[pl.ds(i * 16, 16), 4 * h : 4 * h + 4].astype(F32)
        for n in range(4):
            slab[pl.ds(i * LANES + 4 * h + n, 16, stride=8), :] = rows[:, n]
        return carry

    lax.fori_loop(0, 8, step, 0)


def per_device(frames, w_in, short_taps, filter_taps, skip_gain, w_out):
    vmem = pl.BlockSpec(memory_space=pltpu.VMEM)
    hbm = pl.BlockSpec(memory_space=pl.ANY)
    dma = pltpu.SemaphoreType.DMA
    row, rowi, tc, ts, cc, cs = tables()
    slabs = pltpu.VMEM((ROWS, 8, LANES), BF16)
    scratch = [
        pltpu.VMEM((3, 1024, 256), BF16), pltpu.VMEM((1024, 256), BF16),
        pltpu.VMEM((256, 128), BF16), pltpu.VMEM((128, 256), BF16),
        pltpu.VMEM((128, 512), F32), pltpu.VMEM((128, 512), F32),
        pltpu.VMEM((512, 512), BF16), pltpu.VMEM((512, 512), BF16),
        pltpu.VMEM((4, 512, 256), BF16),
        pltpu.VMEM((528, 768), F32),
        pltpu.VMEM((512, 256), F32), pltpu.VMEM((512, 256), F32),
        pltpu.VMEM((1024, 128), F32),
        slabs, slabs, slabs, slabs, slabs, slabs,
        pltpu.VMEM((16, 768), BF16), pltpu.VMEM((16, 768), BF16),
        pltpu.VMEM((512, 256), BF16),
        pltpu.VMEM((4, 512, 256), BF16),
        pltpu.VMEM((128, 1024), BF16),
        pltpu.VMEM((512, 512), BF16),
        pltpu.VMEM((512, 512), F32),
        pltpu.VMEM((512, 512), F32), pltpu.VMEM((512, 512), F32),
        pltpu.VMEM((256, 512), BF16),
        dma((8,)),
        dma((2,)), dma((2,)), dma((2,)), dma((2,)), dma((2,)), dma((2,)),
        dma((2,)), dma((2,)), dma((2,)), dma((2,)), dma((2,)), dma((2,)),
        dma((4,)), dma((4,)), dma, dma,
    ]
    return pl.pallas_call(
        kernel,
        out_shape=jax.ShapeDtypeStruct(frames.shape, BF16),
        in_specs=[vmem] * 4 + [hbm] * 8,
        out_specs=vmem,
        scratch_shapes=scratch,
        name="hyena",
        compiler_params=pltpu.CompilerParams(
            collective_id=0, has_side_effects=True, vmem_limit_bytes=56 << 20
        ),
    )(frames, filter_taps, short_taps, skip_gain.reshape(1, -1), w_in, w_out, row, rowi, tc, ts, cc, cs)


def solution(mesh):
    return jax.shard_map(
        per_device,
        mesh=mesh,
        in_specs=(
            P("tm", "chan"),
            P(None, None, "chan"),
            P(None, None, "chan"),
            P("tm", "chan"),
            P("chan"),
            P(None, "chan"),
        ),
        out_specs=P("tm", "chan"),
        check_vma=False,
    )
```

```python
import functools

import jax
import jax.numpy as jnp
import numpy as np
from jax import lax
from jax.experimental import pallas as pl
from jax.experimental.pallas import tpu as pltpu
from jax.sharding import PartitionSpec as P

MESH = pl.DeviceIdType.MESH
ROWS = 128
COLS = 512
CHANS = 256
PEERS = ROWS - 1
LANES = 128
HALO = 16
F32 = jnp.float32
BF16 = jnp.bfloat16


def tables():
    r = np.arange(ROWS, dtype=np.int64)
    k = np.arange(ROWS, dtype=np.int64)
    c = np.arange(COLS, dtype=np.int64)
    row = (2.0 * np.pi / (4 * ROWS)) * ((r[None, :] * (4 * k[:, None] + 1)) % (4 * ROWS))
    turn = (2.0 * np.pi / (4 * ROWS * COLS)) * (c[None, :] * (4 * k[:, None] + 1))
    col = (2.0 * np.pi / COLS) * ((c[:, None] * c[None, :]) % COLS)
    row_both = np.concatenate([np.cos(row), -np.sin(row)], axis=0)
    return (
        jnp.asarray(row_both, BF16),
        jnp.asarray(row_both.T, BF16),
        jnp.asarray(np.cos(turn), F32),
        jnp.asarray(np.sin(turn), F32),
        jnp.asarray(np.cos(col), BF16),
        jnp.asarray(np.sin(col), BF16),
    )


def dot(left, right):
    return jnp.dot(left, right, preferred_element_type=F32)


def kernel(
    frames_h, filt_h, taps_h, skip_h, w_in_h, w_out_h, row_h, rowi_h, tc_h, ts_h, cc_h, cs_h,
    out,
    taps, skip, w_in, w_out, row, rowi, tcos, tsin, ccos, csin,
    xg, filt, p, qf, sf, slab, fsend, frecv, ssend, srecv, csend, crecv,
    gbuf, gg, gmat, q2, spec, xm, ym, bstack, acc,
    load_sem, wout_sem, over_s, over_r, near_s, near_r, pass_s, pass_r,
    gover_s, gover_r, gnear_s, gnear_r, gpass_s, gpass_r, a_s, a_r, h_s, h_r,
):
    t = lax.axis_index("tm")
    q = lax.axis_index("chan")
    cross = lax.rem(q + 2, 4)
    sib = q + 1 - 2 * lax.rem(q, 2)
    after = lax.rem(t + 1, ROWS)
    before = lax.rem(t + ROWS - 1, ROWS)
    z = t // 8
    w = t - 8 * z
    inner = [lax.rem(w + j, 8) for j in range(8)]

    def plane(b):
        h = (b + 1) // 2
        zo = 8 + h - 2 * h * lax.rem(b, 2)
        return lax.rem(z + zo, 16) * 8

    def for_peers(act):
        def step(b, carry):
            base = plane(b)
            for j in range(8):
                act(base + inner[j])
            return carry

        lax.fori_loop(0, 15, step, 0)
        for j in range(1, 8):
            act(z * 8 + inner[j])

    pairs = (
        (frames_h, xg.at[q, pl.ds(HALO, COLS)]), (filt_h, filt), (w_in_h, w_in), (taps_h, taps),
        (skip_h, skip), (row_h, row), (tc_h, tcos), (ts_h, tsin), (cc_h, ccos), (cs_h, csin),
        (rowi_h, rowi),
    )
    loads = [pltpu.make_async_copy(a, b, load_sem.at[i]) for i, (a, b) in enumerate(pairs)]
    for e in range(2):
        for n in range(4):
            loads.append(
                pltpu.make_async_copy(
                    w_out_h.at[pl.ds(n * 256 + e * 128, 128)],
                    w_out.at[e, pl.ds(n * 128, 128)],
                    wout_sem.at[4 * e + n],
                )
            )
    for copy in loads[:2]:
        copy.start()

    barrier = pltpu.get_barrier_semaphore()

    def greet(device):
        pl.semaphore_signal(barrier, 1, device_id=device, device_id_type=MESH)

    for_peers(lambda peer: greet({"tm": peer}))
    greet({"chan": cross})
    greet({"chan": sib})
    for n in range(1, 4):
        other = lax.rem(q + n, 4)
        greet({"tm": after, "chan": other})
        greet({"tm": before, "chan": other})

    for copy in loads[2:]:
        copy.start()

    def to_slabs(block_of, cbs, es):
        for e in es:
            for cb in cbs:
                slab[pl.ds(4 * e + cb, ROWS, stride=8), :] = jnp.transpose(block_of(cb, e))

    def pack(send, e):
        def step(i, carry):
            rows = slab[pl.ds(pl.multiple_of(i * LANES, LANES), LANES), :].reshape(16, 8, LANES)
            send[pl.ds(i * 16, 16), 4 * e : 4 * e + 4] = rows[:, 4 * e : 4 * e + 4].astype(BF16)
            return carry

        lax.fori_loop(0, 8, step, 0)

    def unpack(recv, e):
        def step(i, carry):
            rows = recv[pl.ds(i * 16, 16), 4 * e : 4 * e + 4].astype(F32)
            for n in range(4):
                slab[pl.ds(i * LANES + 4 * e + n, 16, stride=8), :] = rows[:, n]
            return carry

        lax.fori_loop(0, 8, step, 0)

    def spread(send, recv, which, e):
        part = pl.ds(4 * e, 4)

        def act(peer):
            pltpu.make_async_remote_copy(
                send.at[peer, part], recv.at[t, part],
                a_s.at[2 * which + e], a_r.at[2 * which + e],
                device_id={"tm": peer}, device_id_type=MESH,
            ).start()

        for_peers(act)
        recv[t, part] = send[t, part]

    def await_recv(recv, which, e):
        part = recv.at[pl.ds(0, PEERS), pl.ds(4 * e, 4)]
        pltpu.make_async_copy(part, part, a_r.at[2 * which + e]).wait()

    def await_send(send, which, e):
        part = send.at[pl.ds(0, PEERS), pl.ds(4 * e, 4)]
        pltpu.make_async_copy(part, part, a_s.at[2 * which + e]).wait()

    loads[1].wait()
    to_slabs(
        lambda cb, e: filt[cb * 128 : cb * 128 + 128, e * 128 : e * 128 + 128].astype(F32),
        range(4), range(2),
    )
    pack(fsend, 0)
    pack(fsend, 1)
    loads[0].wait()
    pl.semaphore_wait(barrier, PEERS + 8)

    def gather_start(src, dst, i, s1, r1, s2, r2):
        made = []
        for peer, s, r in ((cross, s1, r1), (sib, s2, r2)):
            copy = pltpu.make_async_remote_copy(
                src, dst, s.at[i], r.at[i], device_id={"chan": peer}, device_id_type=MESH
            )
            copy.start()
            made.append(copy)
        return made

    def gather_pass(held, i, s3, r3):
        on = pltpu.make_async_remote_copy(
            held, held, s3.at[i], r3.at[i], device_id={"chan": sib}, device_id_type=MESH
        )
        on.start()
        return on

    last = xg.at[q, pl.ds(COLS, HALO)]
    for n in range(4):
        pltpu.make_async_remote_copy(
            last, xg.at[q, pl.ds(0, HALO)], h_s, h_r,
            device_id={"tm": after, "chan": lax.rem(q + n, 4)}, device_id_type=MESH,
        ).start()
    chunk = [pl.ds(HALO + 256 * i, 256) for i in range(2)]
    first = [
        gather_start(xg.at[q, chunk[i]], xg.at[q, chunk[i]], i, over_s, over_r, near_s, near_r)
        for i in range(2)
    ]
    spread(fsend, frecv, 0, 0)
    spread(fsend, frecv, 0, 1)
    loads[2].wait()
    loads[3].wait()
    passed = []
    first[0][0].wait_recv()
    passed.append(gather_pass(xg.at[cross, chunk[0]], 0, pass_s, pass_r))

    def project(low, high):
        for j in range(3):
            total = dot(xg[0, low:high], w_in[j, 0:256])
            for n in range(1, 4):
                total += dot(xg[n, low:high], w_in[j, n * 256 : n * 256 + 256])
            p[low:high, j * 256 : j * 256 + 256] = total.astype(BF16).astype(F32)

    def short(i):
        for base in range(i * 256, i * 256 + 256, 64):
            made = []
            for j in range(3):
                lanes = slice(j * 256, j * 256 + 256)
                made.append(
                    taps[j, 0:1, :] * p[16 + base : 80 + base, lanes]
                    + taps[j, 1:2, :] * p[15 + base : 79 + base, lanes]
                    + taps[j, 2:3, :] * p[14 + base : 78 + base, lanes]
                )
            qf[base : base + 64, :] = made[0]
            sf[base : base + 64, :] = (made[1] * made[2]).astype(BF16).astype(F32)

    edge = xg.at[pl.ds(0, 4), pl.ds(0, HALO)]
    pltpu.make_async_copy(edge, edge, h_r).wait()
    first[0][1].wait_recv()
    passed[0].wait_recv()
    project(0, HALO + 256)
    p[0:HALO, :] = jnp.where(t > 0, p[0:HALO, :], 0.0)
    first[1][0].wait_recv()
    passed.append(gather_pass(xg.at[cross, chunk[1]], 1, pass_s, pass_r))
    block = lambda cb, e: sf[cb * 128 : cb * 128 + 128, e * 128 : e * 128 + 128]
    short(0)
    to_slabs(block, (0, 1), range(2))
    first[1][1].wait_recv()
    passed[1].wait_recv()
    project(HALO + 256, HALO + COLS)
    short(1)
    for e in range(2):
        to_slabs(block, (2, 3), (e,))
        pack(ssend, e)
        spread(ssend, srecv, 1, e)

    for copy in loads[4:]:
        copy.wait()

    def transform(recv, e):
        unpack(recv, e)
        for cb in range(4):
            gmat[:, cb * 128 : cb * 128 + 128] = slab[
                pl.ds(4 * e + cb, ROWS, stride=8), :
            ].astype(BF16)
        both = dot(row[...], gmat[...])
        a, b = both[0:128], both[128:256]
        q2[0:128, :] = (a * tcos[...] + b * tsin[...]).astype(BF16)
        q2[128:256, :] = (b * tcos[...] - a * tsin[...]).astype(BF16)
        xm[...] = dot(q2[...], ccos[...])
        ym[...] = dot(q2[...], csin[...])

    for e in range(2):
        await_recv(frecv, 0, e)
        transform(frecv, e)
        spec[e, 0:128, :] = xm[0:128, :] + ym[128:256, :]
        spec[e, 128:256, :] = xm[128:256, :] - ym[0:128, :]

    for e in range(2):
        await_recv(srecv, 1, e)
        transform(srecv, e)
        sr = xm[0:128, :] + ym[128:256, :]
        si = xm[128:256, :] - ym[0:128, :]
        fr, fi = spec[e, 0:128, :], spec[e, 128:256, :]
        scale = 1.0 / (ROWS * COLS)
        q2[0:128, :] = ((sr * fr - si * fi) * scale).astype(BF16)
        q2[128:256, :] = ((sr * fi + si * fr) * scale).astype(BF16)
        xm[...] = dot(q2[...], ccos[...])
        ym[...] = dot(q2[...], csin[...])
        br = xm[0:128, :] - ym[128:256, :]
        bi = ym[0:128, :] + xm[128:256, :]
        bstack[0:128, :] = (br * tcos[...] - bi * tsin[...]).astype(BF16)
        bstack[128:256, :] = (br * tsin[...] + bi * tcos[...]).astype(BF16)
        conv = dot(rowi[...], bstack[...])
        for cb in range(4):
            slab[pl.ds(4 * e + cb, ROWS, stride=8), :] = conv[:, cb * 128 : cb * 128 + 128]
        pack(csend, e)
        spread(csend, crecv, 2, e)

    second = []
    for e in range(2):
        await_recv(crecv, 2, e)
        unpack(crecv, e)
        lanes = slice(e * 128, e * 128 + 128)
        for cb in range(4):
            rows = slice(cb * 128, cb * 128 + 128)
            conv = jnp.transpose(slab[pl.ds(4 * e + cb, ROWS, stride=8), :])
            gated = qf[rows, lanes] * (conv + skip[:, lanes] * sf[rows, lanes])
            gbuf[e, rows, :] = gated.astype(BF16)
        place = pl.ds(pl.multiple_of(q * 128, 128), 128)
        second.append(
            gather_start(gbuf.at[e], gg.at[e, :, place], e, gover_s, gover_r, gnear_s, gnear_r)
        )
        gg[e, :, place] = gbuf[e]

    onward = []
    for e in range(2):
        second[e][0].wait_recv()
        held = gg.at[e, :, pl.ds(pl.multiple_of(cross * 128, 128), 128)]
        onward.append(gather_pass(held, e, gpass_s, gpass_r))
        second[e][1].wait_recv()
        onward[e].wait_recv()
        total = dot(gg[e], w_out[e])
        if e == 0:
            acc[...] = total + xg[q, HALO : HALO + COLS].astype(F32)
        else:
            out[...] = (acc[...] + total).astype(BF16)

    for e in range(2):
        await_send(fsend, 0, e)
        await_send(ssend, 1, e)
        await_send(csend, 2, e)
    pltpu.make_async_copy(edge, edge, h_s).wait()
    for copies in first + second:
        for copy in copies:
            copy.wait_send()
    for copy in passed + onward:
        copy.wait_send()


def per_device(frames, w_in, short_taps, filter_taps, skip_gain, w_out):
    vmem = pl.BlockSpec(memory_space=pltpu.VMEM)
    hbm = pl.BlockSpec(memory_space=pl.ANY)
    dma = pltpu.SemaphoreType.DMA
    row, rowi, tc, ts, cc, cs = tables()
    slabs = pltpu.VMEM((ROWS, 8, LANES), BF16)
    scratch = [
        pltpu.VMEM((3, 3, 256), F32), pltpu.VMEM((1, 256), F32),
        pltpu.VMEM((3, 1024, 256), BF16), pltpu.VMEM((2, 512, 256), BF16),
        pltpu.VMEM((256, 128), BF16), pltpu.VMEM((128, 256), BF16),
        pltpu.VMEM((128, 512), F32), pltpu.VMEM((128, 512), F32),
        pltpu.VMEM((512, 512), BF16), pltpu.VMEM((512, 512), BF16),
        pltpu.VMEM((4, HALO + COLS, 256), BF16),
        pltpu.VMEM((512, 256), BF16),
        pltpu.VMEM((HALO + COLS, 768), F32),
        pltpu.VMEM((512, 256), F32), pltpu.VMEM((512, 256), F32),
        pltpu.VMEM((1024, 128), F32),
        slabs, slabs, slabs, slabs, slabs, slabs,
        pltpu.VMEM((2, 512, 128), BF16),
        pltpu.VMEM((2, 512, 512), BF16),
        pltpu.VMEM((128, 512), BF16),
        pltpu.VMEM((256, 512), BF16),
        pltpu.VMEM((2, 256, 512), F32),
        pltpu.VMEM((256, 512), F32), pltpu.VMEM((256, 512), F32),
        pltpu.VMEM((256, 512), BF16),
        pltpu.VMEM((512, 256), F32),
        dma((11,)), dma((8,)),
    ] + [dma((2,))] * 12 + [dma((6,)), dma((6,)), dma, dma]
    return pl.pallas_call(
        kernel,
        out_shape=jax.ShapeDtypeStruct(frames.shape, BF16),
        in_specs=[hbm] * 12,
        out_specs=vmem,
        scratch_shapes=scratch,
        name="hyena",
        compiler_params=pltpu.CompilerParams(
            collective_id=0, has_side_effects=True, vmem_limit_bytes=60 << 20
        ),
    )(frames, filter_taps, short_taps, skip_gain.reshape(1, -1), w_in, w_out, row, rowi, tc, ts, cc, cs)


def solution(mesh):
    return jax.shard_map(
        per_device,
        mesh=mesh,
        in_specs=(
            P("tm", "chan"),
            P(None, None, "chan"),
            P(None, None, "chan"),
            P("tm", "chan"),
            P("chan"),
            P(None, "chan"),
        ),
        out_specs=P("tm", "chan"),
        check_vma=False,
    )
```

```python
import functools

import jax
import jax.numpy as jnp
import numpy as np
from jax import lax
from jax.experimental import pallas as pl
from jax.experimental.pallas import tpu as pltpu
from jax.sharding import PartitionSpec as P

MESH = pl.DeviceIdType.MESH
ROWS = 128
COLS = 512
CHANS = 256
PEERS = ROWS - 1
LANES = 128
HALO = 16
F32 = jnp.float32
BF16 = jnp.bfloat16


def tables():
    r = np.arange(ROWS, dtype=np.int64)
    k = np.arange(ROWS, dtype=np.int64)
    c = np.arange(COLS, dtype=np.int64)
    row = (2.0 * np.pi / (4 * ROWS)) * ((r[None, :] * (4 * k[:, None] + 1)) % (4 * ROWS))
    turn = (2.0 * np.pi / (4 * ROWS * COLS)) * (c[None, :] * (4 * k[:, None] + 1))
    col = (2.0 * np.pi / COLS) * ((c[:, None] * c[None, :]) % COLS)
    row_both = np.concatenate([np.cos(row), -np.sin(row)], axis=0)
    return (
        jnp.asarray(row_both, BF16),
        jnp.asarray(row_both.T, BF16),
        jnp.asarray(np.cos(turn), F32),
        jnp.asarray(np.sin(turn), F32),
        jnp.asarray(np.cos(col), BF16),
        jnp.asarray(np.sin(col), BF16),
    )


def dot(left, right):
    return jnp.dot(left, right, preferred_element_type=F32)


def kernel(
    frames_h, filt_h, taps_h, skip_h, w_in_h, w_out_h, row_h, rowi_h, tc_h, ts_h, cc_h, cs_h,
    out,
    taps, skip, w_in, w_out, row, rowi, tcos, tsin, ccos, csin,
    xg, filt, p, qf, sf, slab, fsend, frecv, ssend, srecv, csend, crecv,
    gbuf, gg, gmat, q2, spec, xm, ym, bstack, acc,
    load_sem, wout_sem, over_s, over_r, near_s, near_r, pass_s, pass_r,
    gover_s, gover_r, gnear_s, gnear_r, gpass_s, gpass_r, a_s, a_r, h_s, h_r,
):
    t = lax.axis_index("tm")
    q = lax.axis_index("chan")
    cross = lax.rem(q + 2, 4)
    sib = q + 1 - 2 * lax.rem(q, 2)
    after = lax.rem(t + 1, ROWS)
    before = lax.rem(t + ROWS - 1, ROWS)
    z = t // 8
    w = t - 8 * z
    inner = [lax.rem(w + j, 8) for j in range(8)]

    def plane(b):
        h = (b + 1) // 2
        zo = 8 + h - 2 * h * lax.rem(b, 2)
        return lax.rem(z + zo, 16) * 8

    def for_peers(act, chosen=range(8)):
        def step(b, carry):
            base = plane(b)
            for j in chosen:
                act(base + inner[j])
            return carry

        lax.fori_loop(0, 15, step, 0)
        for j in chosen:
            if j > 0:
                act(z * 8 + inner[j])

    pairs = (
        (frames_h, xg.at[q, pl.ds(HALO, COLS)]), (filt_h, filt), (w_in_h, w_in), (taps_h, taps),
        (skip_h, skip), (row_h, row), (tc_h, tcos), (ts_h, tsin), (cc_h, ccos), (cs_h, csin),
        (rowi_h, rowi),
    )
    loads = [pltpu.make_async_copy(a, b, load_sem.at[i]) for i, (a, b) in enumerate(pairs)]
    for e in range(2):
        for n in range(4):
            loads.append(
                pltpu.make_async_copy(
                    w_out_h.at[pl.ds(n * 256 + e * 128, 128)],
                    w_out.at[e, pl.ds(n * 128, 128)],
                    wout_sem.at[4 * e + n],
                )
            )
    for copy in loads[:2]:
        copy.start()

    barrier = pltpu.get_barrier_semaphore()

    def greet(device):
        pl.semaphore_signal(barrier, 1, device_id=device, device_id_type=MESH)

    for_peers(lambda peer: greet({"tm": peer}))
    greet({"chan": cross})
    greet({"chan": sib})
    for n in range(1, 4):
        other = lax.rem(q + n, 4)
        greet({"tm": after, "chan": other})
        greet({"tm": before, "chan": other})

    for copy in loads[2:]:
        copy.start()

    def to_slabs(block_of, cbs, es):
        for e in es:
            for cb in cbs:
                slab[pl.ds(4 * e + cb, ROWS, stride=8), :] = jnp.transpose(block_of(cb, e))

    def pack(send, e):
        def step(i, carry):
            rows = slab[pl.ds(pl.multiple_of(i * LANES, LANES), LANES), :].reshape(16, 8, LANES)
            send[pl.ds(i * 16, 16), 4 * e : 4 * e + 4] = rows[:, 4 * e : 4 * e + 4].astype(BF16)
            return carry

        lax.fori_loop(0, 8, step, 0)

    def unpack(recv, e, low=0, high=4):
        def step(i, carry):
            rows = recv[pl.ds(i * 16, 16), 4 * e + low : 4 * e + high].astype(F32)
            for n in range(high - low):
                slab[pl.ds(i * LANES + 4 * e + low + n, 16, stride=8), :] = rows[:, n]
            return carry

        lax.fori_loop(0, 8, step, 0)

    def spread(send, recv, which, part, walk=for_peers):
        def act(peer):
            pltpu.make_async_remote_copy(
                send.at[peer, part], recv.at[t, part], a_s.at[which], a_r.at[which],
                device_id={"tm": peer}, device_id_type=MESH,
            ).start()

        walk(act)

    def await_all(held, part, sem):
        some = held.at[pl.ds(0, PEERS), part]
        pltpu.make_async_copy(some, some, sem).wait()

    WHOLE = pl.ds(0, 8)
    HALF = (pl.ds(0, 4), pl.ds(4, 4))
    PIECES = ((0, 0, 4), (1, 0, 4))
    PARTS = [pl.ds(4 * e + low, high - low) for e, low, high in PIECES]

    loads[1].wait()
    to_slabs(
        lambda cb, e: filt[cb * 128 : cb * 128 + 128, e * 128 : e * 128 + 128].astype(F32),
        range(4), range(2),
    )
    pack(fsend, 0)
    pack(fsend, 1)
    loads[0].wait()
    pl.semaphore_wait(barrier, PEERS + 8)

    def gather_start(src, dst, i, s1, r1, s2, r2):
        made = []
        for peer, s, r in ((cross, s1, r1), (sib, s2, r2)):
            copy = pltpu.make_async_remote_copy(
                src, dst, s.at[i], r.at[i], device_id={"chan": peer}, device_id_type=MESH
            )
            copy.start()
            made.append(copy)
        return made

    def gather_pass(held, i, s3, r3):
        on = pltpu.make_async_remote_copy(
            held, held, s3.at[i], r3.at[i], device_id={"chan": sib}, device_id_type=MESH
        )
        on.start()
        return on

    last = xg.at[q, pl.ds(COLS, HALO)]
    for n in range(4):
        pltpu.make_async_remote_copy(
            last, xg.at[q, pl.ds(0, HALO)], h_s, h_r,
            device_id={"tm": after, "chan": lax.rem(q + n, 4)}, device_id_type=MESH,
        ).start()
    chunk = [pl.ds(HALO + 256 * i, 256) for i in range(2)]
    first = [
        gather_start(xg.at[q, chunk[i]], xg.at[q, chunk[i]], i, over_s, over_r, near_s, near_r)
        for i in range(2)
    ]
    spread(fsend, frecv, 0, WHOLE, lambda act: for_peers(act, (0, 2, 4, 6)))
    frecv[t] = fsend[t]
    passed = []
    first[0][0].wait_recv()
    passed.append(gather_pass(xg.at[cross, chunk[0]], 0, pass_s, pass_r))
    spread(fsend, frecv, 0, WHOLE, lambda act: for_peers(act, (1, 3, 5, 7)))
    loads[2].wait()
    loads[3].wait()

    def short(i):
        for base in range(i * 256, i * 256 + 256, 64):
            made = []
            for j in range(3):
                lanes = slice(j * 256, j * 256 + 256)
                made.append(
                    taps[j, 0:1, :] * p[16 + base : 80 + base, lanes]
                    + taps[j, 1:2, :] * p[15 + base : 79 + base, lanes]
                    + taps[j, 2:3, :] * p[14 + base : 78 + base, lanes]
                )
            qf[base : base + 64, :] = made[0]
            sf[base : base + 64, :] = (made[1] * made[2]).astype(BF16).astype(F32)

    edge = xg.at[pl.ds(0, 4), pl.ds(0, HALO)]
    diagonal = lax.rem(sib + 2, 4)
    block = lambda cb, e: sf[cb * 128 : cb * 128 + 128, e * 128 : e * 128 + 128]
    spans = ((0, HALO + 256), (HALO + 256, HALO + COLS))

    def add_product(i, n, state):
        low, high = spans[i]
        held = xg[n, low:high]
        for j in range(3):
            lanes = slice(j * 256, j * 256 + 256)
            total = dot(held, w_in[j, pl.ds(pl.multiple_of(n * 256, 256), 256)])
            if state > 0:
                total += p[low:high, lanes]
            if state == 2:
                total = total.astype(BF16).astype(F32)
            p[low:high, lanes] = total

    pltpu.make_async_copy(edge, edge, h_r).wait()
    for i in range(2):
        add_product(i, q, 0)
        first[i][1].wait_recv()
        add_product(i, sib, 1)
        if i == 1:
            first[1][0].wait_recv()
            passed.append(gather_pass(xg.at[cross, chunk[1]], 1, pass_s, pass_r))
        add_product(i, cross, 1)
        if i == 1:
            short(0)
            to_slabs(block, (0, 1), range(2))
        passed[i].wait_recv()
        add_product(i, diagonal, 2)
        if i == 0:
            p[0:HALO, :] = jnp.where(t > 0, p[0:HALO, :], 0.0)
    short(1)
    for e in range(2):
        to_slabs(block, (2, 3), (e,))
        pack(ssend, e)
        spread(ssend, srecv, 1 + e, HALF[e])
        srecv[t, HALF[e]] = ssend[t, HALF[e]]

    for copy in loads[4:]:
        copy.wait()

    def transform(recv, e):
        unpack(recv, e)
        for cb in range(4):
            gmat[:, cb * 128 : cb * 128 + 128] = slab[
                pl.ds(4 * e + cb, ROWS, stride=8), :
            ].astype(BF16)
        both = dot(row[...], gmat[...])
        a, b = both[0:128], both[128:256]
        q2[0:128, :] = (a * tcos[...] + b * tsin[...]).astype(BF16)
        q2[128:256, :] = (b * tcos[...] - a * tsin[...]).astype(BF16)
        xm[...] = dot(q2[...], ccos[...])
        ym[...] = dot(q2[...], csin[...])

    await_all(frecv, WHOLE, a_r.at[0])
    for e in range(2):
        transform(frecv, e)
        spec[e, 0:128, :] = xm[0:128, :] + ym[128:256, :]
        spec[e, 128:256, :] = xm[128:256, :] - ym[0:128, :]

    for e in range(2):
        await_all(srecv, HALF[e], a_r.at[1 + e])
        transform(srecv, e)
        sr = xm[0:128, :] + ym[128:256, :]
        si = xm[128:256, :] - ym[0:128, :]
        fr, fi = spec[e, 0:128, :], spec[e, 128:256, :]
        scale = 1.0 / (ROWS * COLS)
        q2[0:128, :] = ((sr * fr - si * fi) * scale).astype(BF16)
        q2[128:256, :] = ((sr * fi + si * fr) * scale).astype(BF16)
        xm[...] = dot(q2[...], ccos[...])
        ym[...] = dot(q2[...], csin[...])
        br = xm[0:128, :] - ym[128:256, :]
        bi = ym[0:128, :] + xm[128:256, :]
        bstack[0:128, :] = (br * tcos[...] - bi * tsin[...]).astype(BF16)
        bstack[128:256, :] = (br * tsin[...] + bi * tcos[...]).astype(BF16)
        conv = dot(rowi[...], bstack[...])
        for cb in range(4):
            slab[pl.ds(4 * e + cb, ROWS, stride=8), :] = conv[:, cb * 128 : cb * 128 + 128]
        pack(csend, e)
        for i, piece in enumerate(PIECES):
            if piece[0] == e:
                spread(csend, crecv, 3 + i, PARTS[i])
        crecv[t, HALF[e]] = csend[t, HALF[e]]

    second, onward = [], []
    place = pl.ds(pl.multiple_of(q * 128, 128), 128)
    cross_place = pl.ds(pl.multiple_of(cross * 128, 128), 128)

    def returned(i):
        e, low, high = PIECES[i]
        await_all(crecv, PARTS[i], a_r.at[3 + i])
        unpack(crecv, e, low, high)
        lanes = slice(e * 128, e * 128 + 128)
        for cb in range(low, high):
            rows = slice(cb * 128, cb * 128 + 128)
            conv = jnp.transpose(slab[pl.ds(4 * e + cb, ROWS, stride=8), :])
            gated = qf[rows, lanes] * (conv + skip[:, lanes] * sf[rows, lanes])
            gbuf[e, rows, :] = gated.astype(BF16)
        rows = pl.ds(low * 128, (high - low) * 128)
        second.append(
            gather_start(
                gbuf.at[e, rows], gg.at[e, rows, place], i, gover_s, gover_r, gnear_s, gnear_r
            )
        )
        gg[e, rows, place] = gbuf[e, rows]

    def forward(i):
        e, low, high = PIECES[i]
        second[i][0].wait_recv()
        held = gg.at[e, pl.ds(low * 128, (high - low) * 128), cross_place]
        onward.append(gather_pass(held, i, gpass_s, gpass_r))

    def mixed(i):
        e, low, high = PIECES[i]
        rows = slice(low * 128, high * 128)
        second[i][1].wait_recv()
        onward[i].wait_recv()
        return rows, dot(gg[e, rows], w_out[e])

    returned(0)
    forward(0)
    returned(1)
    rows, total = mixed(0)
    acc[rows, :] = total + xg[q, HALO : HALO + COLS].astype(F32)
    forward(1)
    rows, total = mixed(1)
    out[rows, :] = (acc[rows, :] + total).astype(BF16)

    await_all(fsend, WHOLE, a_s.at[0])
    for e in range(2):
        await_all(ssend, HALF[e], a_s.at[1 + e])
    for i in range(2):
        await_all(csend, PARTS[i], a_s.at[3 + i])
    pltpu.make_async_copy(edge, edge, h_s).wait()
    for copies in first + second:
        for copy in copies:
            copy.wait_send()
    for copy in passed + onward:
        copy.wait_send()


def per_device(frames, w_in, short_taps, filter_taps, skip_gain, w_out):
    vmem = pl.BlockSpec(memory_space=pltpu.VMEM)
    hbm = pl.BlockSpec(memory_space=pl.ANY)
    dma = pltpu.SemaphoreType.DMA
    row, rowi, tc, ts, cc, cs = tables()
    operands = (
        frames, filter_taps, short_taps, skip_gain.reshape(1, -1), w_in, w_out,
        row, rowi, tc, ts, cc, cs,
    )
    slabs = pltpu.VMEM((ROWS, 8, LANES), BF16)
    scratch = [
        pltpu.VMEM((3, 3, 256), F32), pltpu.VMEM((1, 256), F32),
        pltpu.VMEM((3, 1024, 256), BF16), pltpu.VMEM((2, 512, 256), BF16),
        pltpu.VMEM((256, 128), BF16), pltpu.VMEM((128, 256), BF16),
        pltpu.VMEM((128, 512), F32), pltpu.VMEM((128, 512), F32),
        pltpu.VMEM((512, 512), BF16), pltpu.VMEM((512, 512), BF16),
        pltpu.VMEM((4, HALO + COLS, 256), BF16),
        pltpu.VMEM((512, 256), BF16),
        pltpu.VMEM((HALO + COLS, 768), F32),
        pltpu.VMEM((512, 256), F32), pltpu.VMEM((512, 256), F32),
        pltpu.VMEM((1024, 128), F32),
        slabs, slabs, slabs, slabs, slabs, slabs,
        pltpu.VMEM((2, 512, 128), BF16),
        pltpu.VMEM((2, 512, 512), BF16),
        pltpu.VMEM((128, 512), BF16),
        pltpu.VMEM((256, 512), BF16),
        pltpu.VMEM((2, 256, 512), F32),
        pltpu.VMEM((256, 512), F32), pltpu.VMEM((256, 512), F32),
        pltpu.VMEM((256, 512), BF16),
        pltpu.VMEM((512, 256), F32),
        dma((11,)), dma((8,)),
    ] + [dma((2,))] * 6 + [dma((3,))] * 6 + [dma((6,)), dma((6,)), dma, dma]
    return pl.pallas_call(
        kernel,
        out_shape=jax.ShapeDtypeStruct(frames.shape, BF16),
        in_specs=[hbm] * 12,
        out_specs=vmem,
        scratch_shapes=scratch,
        name="hyena",
        compiler_params=pltpu.CompilerParams(
            collective_id=0, has_side_effects=True, vmem_limit_bytes=30 << 20
        ),
    )(*[pltpu.with_memory_space_constraint(v, pltpu.HBM) for v in operands])


def solution(mesh):
    return jax.shard_map(
        per_device,
        mesh=mesh,
        in_specs=(
            P("tm", "chan"),
            P(None, None, "chan"),
            P(None, None, "chan"),
            P("tm", "chan"),
            P("chan"),
            P(None, "chan"),
        ),
        out_specs=P("tm", "chan"),
        check_vma=False,
    )
```

```python
import functools

import jax
import jax.numpy as jnp
import numpy as np
from jax import lax
from jax.experimental import pallas as pl
from jax.experimental.pallas import tpu as pltpu
from jax.sharding import PartitionSpec as P

MESH = pl.DeviceIdType.MESH
ROWS = 128
COLS = 512
CHANS = 256
PEERS = ROWS - 1
LANES = 128
EARLY = 2
HALO = 16
F32 = jnp.float32
BF16 = jnp.bfloat16


def tables():
    r = np.arange(ROWS, dtype=np.int64)
    k = np.arange(ROWS, dtype=np.int64)
    c = np.arange(COLS, dtype=np.int64)
    row = (2.0 * np.pi / (4 * ROWS)) * ((r[None, :] * (4 * k[:, None] + 1)) % (4 * ROWS))
    turn = (2.0 * np.pi / (4 * ROWS * COLS)) * (c[None, :] * (4 * k[:, None] + 1))
    col = (2.0 * np.pi / COLS) * ((c[:, None] * c[None, :]) % COLS)
    row_both = np.concatenate([np.cos(row), -np.sin(row)], axis=0)
    return (
        jnp.asarray(row_both, BF16),
        jnp.asarray(row_both.T, BF16),
        jnp.asarray(np.cos(turn), F32),
        jnp.asarray(np.sin(turn), F32),
        jnp.asarray(np.cos(col), BF16),
        jnp.asarray(np.sin(col), BF16),
    )


def dot(left, right):
    return jnp.dot(left, right, preferred_element_type=F32)


def kernel(
    frames_h, filt_h, taps_h, skip_h, w_in_h, w_out_h, row_h, rowi_h, tc_h, ts_h, cc_h, cs_h,
    out,
    taps, skip, w_in, w_out, row, rowi, tcos, tsin, ccos, csin,
    xg, filt, p, qf, sf, slab, fsend, frecv, ssend, srecv, csend, crecv,
    gbuf, gg, gmat, q2, spec, xm, ym, bstack, acc,
    load_sem, wout_sem, over_s, over_r, near_s, near_r, pass_s, pass_r,
    gover_s, gover_r, gnear_s, gnear_r, gpass_s, gpass_r, a_s, a_r, h_s, h_r, last_s,
):
    t = lax.axis_index("tm")
    q = lax.axis_index("chan")
    cross = lax.rem(q + 2, 4)
    sib = q + 1 - 2 * lax.rem(q, 2)
    after = lax.rem(t + 1, ROWS)
    before = lax.rem(t + ROWS - 1, ROWS)
    z = t // 8
    w = t - 8 * z
    inner = [lax.rem(w + j, 8) for j in range(8)]

    def plane(b):
        h = (b + 1) // 2
        zo = 8 + h - 2 * h * lax.rem(b, 2)
        return lax.rem(z + zo, 16) * 8

    def for_peers(act, chosen=range(8)):
        def step(b, carry):
            base = plane(b)
            for j in chosen:
                act(base + inner[j])
            return carry

        lax.fori_loop(0, 15, step, 0)
        for j in chosen:
            if j > 0:
                act(z * 8 + inner[j])

    def for_peers_early(act):
        for other in range(EARLY):

            @pl.when(z != other)
            def _():
                for j in range(8):
                    act(other * 8 + inner[j])

        def step(b, carry):
            base = plane(b)

            @pl.when(base >= EARLY * 8)
            def _():
                for j in range(8):
                    act(base + inner[j])

            return carry

        lax.fori_loop(0, 15, step, 0)
        for j in range(1, 8):
            act(z * 8 + inner[j])

    pairs = (
        (frames_h, xg.at[q, pl.ds(HALO, COLS)]), (filt_h, filt), (w_in_h, w_in), (taps_h, taps),
        (skip_h, skip), (row_h, row), (tc_h, tcos), (ts_h, tsin), (cc_h, ccos), (cs_h, csin),
        (rowi_h, rowi),
    )
    loads = [pltpu.make_async_copy(a, b, load_sem.at[i]) for i, (a, b) in enumerate(pairs)]
    for e in range(2):
        for n in range(4):
            loads.append(
                pltpu.make_async_copy(
                    w_out_h.at[pl.ds(n * 256 + e * 128, 128)],
                    w_out.at[e, pl.ds(n * 128, 128)],
                    wout_sem.at[4 * e + n],
                )
            )
    for copy in loads[:2]:
        copy.start()

    barrier = pltpu.get_barrier_semaphore()

    def greet(device):
        pl.semaphore_signal(barrier, 1, device_id=device, device_id_type=MESH)

    for_peers(lambda peer: greet({"tm": peer}))
    greet({"chan": cross})
    greet({"chan": sib})
    for n in range(1, 4):
        other = lax.rem(q + n, 4)
        greet({"tm": after, "chan": other})
        greet({"tm": before, "chan": other})

    for copy in loads[2:]:
        copy.start()

    def to_slabs(block_of, cbs, es):
        for e in es:
            for cb in cbs:
                slab[pl.ds(4 * e + cb, ROWS, stride=8), :] = jnp.transpose(block_of(cb, e))

    def pack(send, e):
        def step(i, carry):
            rows = slab[pl.ds(pl.multiple_of(i * LANES, LANES), LANES), :].reshape(16, 8, LANES)
            send[pl.ds(i * 16, 16), 4 * e : 4 * e + 4] = rows[:, 4 * e : 4 * e + 4].astype(BF16)
            return carry

        lax.fori_loop(0, 8, step, 0)

    def unpack(recv, e, low=0, high=4):
        def step(i, carry):
            rows = recv[pl.ds(i * 16, 16), 4 * e + low : 4 * e + high].astype(F32)
            for n in range(high - low):
                slab[pl.ds(i * LANES + 4 * e + low + n, 16, stride=8), :] = rows[:, n]
            return carry

        lax.fori_loop(0, 8, step, 0)

    def spread(send, recv, which, part, walk=for_peers):
        def act(peer):
            pltpu.make_async_remote_copy(
                send.at[peer, part], recv.at[t, part], a_s.at[which], a_r.at[which],
                device_id={"tm": peer}, device_id_type=MESH,
            ).start()

        walk(act)

    def await_all(held, part, sem):
        some = held.at[pl.ds(0, PEERS), part]
        pltpu.make_async_copy(some, some, sem).wait()

    WHOLE = pl.ds(0, 8)
    HALF = (pl.ds(0, 4), pl.ds(4, 4))
    PIECES = ((0, 0, 4), (1, 0, 4))
    PARTS = [pl.ds(4 * e + low, high - low) for e, low, high in PIECES]

    loads[1].wait()
    to_slabs(
        lambda cb, e: filt[cb * 128 : cb * 128 + 128, e * 128 : e * 128 + 128].astype(F32),
        range(4), range(2),
    )
    pack(fsend, 0)
    pack(fsend, 1)
    loads[0].wait()
    pl.semaphore_wait(barrier, PEERS + 8)

    def gather_start(src, dst, i, s1, r1, s2, r2):
        made = []
        for peer, s, r in ((cross, s1, r1), (sib, s2, r2)):
            copy = pltpu.make_async_remote_copy(
                src, dst, s.at[i], r.at[i], device_id={"chan": peer}, device_id_type=MESH
            )
            copy.start()
            made.append(copy)
        return made

    def gather_pass(held, i, s3, r3):
        on = pltpu.make_async_remote_copy(
            held, held, s3.at[i], r3.at[i], device_id={"chan": sib}, device_id_type=MESH
        )
        on.start()
        return on

    last = xg.at[q, pl.ds(COLS, HALO)]
    for n in range(4):
        pltpu.make_async_remote_copy(
            last, xg.at[q, pl.ds(0, HALO)], h_s, h_r,
            device_id={"tm": after, "chan": lax.rem(q + n, 4)}, device_id_type=MESH,
        ).start()
    chunk = [pl.ds(HALO + 256 * i, 256) for i in range(2)]
    first = [
        gather_start(xg.at[q, chunk[i]], xg.at[q, chunk[i]], i, over_s, over_r, near_s, near_r)
        for i in range(2)
    ]
    spread(fsend, frecv, 0, WHOLE, lambda act: for_peers(act, (0, 2, 4, 6, 1)))
    frecv[t] = fsend[t]
    passed = []
    first[0][0].wait_recv()
    passed.append(gather_pass(xg.at[cross, chunk[0]], 0, pass_s, pass_r))
    spread(fsend, frecv, 0, WHOLE, lambda act: for_peers(act, (3, 5, 7)))
    loads[2].wait()
    loads[3].wait()

    def short(i):
        for base in range(i * 256, i * 256 + 256, 64):
            made = []
            for j in range(3):
                lanes = slice(j * 256, j * 256 + 256)
                made.append(
                    taps[j, 0:1, :] * p[16 + base : 80 + base, lanes]
                    + taps[j, 1:2, :] * p[15 + base : 79 + base, lanes]
                    + taps[j, 2:3, :] * p[14 + base : 78 + base, lanes]
                )
            qf[base : base + 64, :] = made[0]
            sf[base : base + 64, :] = (made[1] * made[2]).astype(BF16).astype(F32)

    edge = xg.at[pl.ds(0, 4), pl.ds(0, HALO)]
    diagonal = lax.rem(sib + 2, 4)
    block = lambda cb, e: sf[cb * 128 : cb * 128 + 128, e * 128 : e * 128 + 128]
    spans = ((0, HALO + 256), (HALO + 256, HALO + COLS))

    def add_product(i, n, state):
        low, high = spans[i]
        held = xg[n, low:high]
        for j in range(3):
            lanes = slice(j * 256, j * 256 + 256)
            total = dot(held, w_in[j, pl.ds(pl.multiple_of(n * 256, 256), 256)])
            if state > 0:
                total += p[low:high, lanes]
            if state == 2:
                total = total.astype(BF16).astype(F32)
            p[low:high, lanes] = total

    pltpu.make_async_copy(edge, edge, h_r).wait()
    for i in range(2):
        add_product(i, q, 0)
        first[i][1].wait_recv()
        add_product(i, sib, 1)
        if i == 1:
            first[1][0].wait_recv()
            passed.append(gather_pass(xg.at[cross, chunk[1]], 1, pass_s, pass_r))
        add_product(i, cross, 1)
        if i == 1:
            short(0)
            to_slabs(block, (0, 1), range(2))
        passed[i].wait_recv()
        add_product(i, diagonal, 2)
        if i == 0:
            p[0:HALO, :] = jnp.where(t > 0, p[0:HALO, :], 0.0)
    short(1)
    for e in range(2):
        to_slabs(block, (2, 3), (e,))
        pack(ssend, e)
        spread(ssend, srecv, 1 + e, HALF[e])
        srecv[t, HALF[e]] = ssend[t, HALF[e]]

    for copy in loads[4:]:
        copy.wait()

    def transform(recv, e):
        unpack(recv, e)
        for cb in range(4):
            gmat[:, cb * 128 : cb * 128 + 128] = slab[
                pl.ds(4 * e + cb, ROWS, stride=8), :
            ].astype(BF16)
        both = dot(row[...], gmat[...])
        a, b = both[0:128], both[128:256]
        q2[0:128, :] = (a * tcos[...] + b * tsin[...]).astype(BF16)
        q2[128:256, :] = (b * tcos[...] - a * tsin[...]).astype(BF16)
        xm[...] = dot(q2[...], ccos[...])
        ym[...] = dot(q2[...], csin[...])

    await_all(frecv, WHOLE, a_r.at[0])
    for e in range(2):
        transform(frecv, e)
        spec[e, 0:128, :] = xm[0:128, :] + ym[128:256, :]
        spec[e, 128:256, :] = xm[128:256, :] - ym[0:128, :]

    for e in range(2):
        await_all(srecv, HALF[e], a_r.at[1 + e])
        transform(srecv, e)
        sr = xm[0:128, :] + ym[128:256, :]
        si = xm[128:256, :] - ym[0:128, :]
        fr, fi = spec[e, 0:128, :], spec[e, 128:256, :]
        scale = 1.0 / (ROWS * COLS)
        q2[0:128, :] = ((sr * fr - si * fi) * scale).astype(BF16)
        q2[128:256, :] = ((sr * fi + si * fr) * scale).astype(BF16)
        xm[...] = dot(q2[...], ccos[...])
        ym[...] = dot(q2[...], csin[...])
        br = xm[0:128, :] - ym[128:256, :]
        bi = ym[0:128, :] + xm[128:256, :]
        bstack[0:128, :] = (br * tcos[...] - bi * tsin[...]).astype(BF16)
        bstack[128:256, :] = (br * tsin[...] + bi * tcos[...]).astype(BF16)
        conv = dot(rowi[...], bstack[...])
        for cb in range(4):
            slab[pl.ds(4 * e + cb, ROWS, stride=8), :] = conv[:, cb * 128 : cb * 128 + 128]
        pack(csend, e)
        for i, piece in enumerate(PIECES):
            if piece[0] == e:
                walk = for_peers_early if e == 1 else for_peers
                spread(csend, crecv, 3 + i, PARTS[i], walk)
        crecv[t, HALF[e]] = csend[t, HALF[e]]

    second, onward = [], []
    place = pl.ds(pl.multiple_of(q * 128, 128), 128)
    cross_place = pl.ds(pl.multiple_of(cross * 128, 128), 128)
    sib_place = pl.ds(pl.multiple_of(sib * 128, 128), 128)

    def returned(i):
        e, low, high = PIECES[i]
        await_all(crecv, PARTS[i], a_r.at[3 + i])
        unpack(crecv, e, low, high)
        lanes = slice(e * 128, e * 128 + 128)
        for cb in range(low, high):
            rows = slice(cb * 128, cb * 128 + 128)
            conv = jnp.transpose(slab[pl.ds(4 * e + cb, ROWS, stride=8), :])
            gated = qf[rows, lanes] * (conv + skip[:, lanes] * sf[rows, lanes])
            gbuf[e, rows, :] = gated.astype(BF16)
        rows = pl.ds(low * 128, (high - low) * 128)
        second.append(
            gather_start(
                gbuf.at[e, rows], gg.at[e, rows, place], i, gover_s, gover_r, gnear_s, gnear_r
            )
        )
        gg[e, rows, place] = gbuf[e, rows]

    def forward(i):
        e, low, high = PIECES[i]
        second[i][0].wait_recv()
        held = gg.at[e, pl.ds(low * 128, (high - low) * 128), cross_place]
        onward.append(gather_pass(held, i, gpass_s, gpass_r))

    def mixed(i):
        e, low, high = PIECES[i]
        rows = slice(low * 128, high * 128)
        second[i][1].wait_recv()
        onward[i].wait_recv()
        return rows, dot(gg[e, rows], w_out[e])

    returned(0)
    forward(0)
    returned(1)
    rows, total = mixed(0)
    acc[rows, :] = total + xg[q, HALO : HALO + COLS].astype(F32)
    second[1][0].wait_recv()
    relays = [
        pltpu.make_async_remote_copy(
            gg.at[1, :, source], gg.at[1, :, source], sem, gpass_r.at[1],
            device_id={"chan": peer}, device_id_type=MESH,
        )
        for source, sem, peer in (
            (cross_place, gpass_s.at[1], sib), (sib_place, last_s, cross)
        )
    ]

    @pl.when(lax.rem(q, 2) == 1)
    def _():
        relays[0].start()
        second[1][1].wait_recv()
        relays[1].start()

    @pl.when(lax.rem(q, 2) == 0)
    def _():
        second[1][1].wait_recv()

    relays[0].wait_recv()
    rows, total = slice(0, 512), dot(gg[1], w_out[1])
    out[rows, :] = (acc[rows, :] + total).astype(BF16)

    await_all(fsend, WHOLE, a_s.at[0])
    for e in range(2):
        await_all(ssend, HALF[e], a_s.at[1 + e])
    for i in range(2):
        await_all(csend, PARTS[i], a_s.at[3 + i])
    pltpu.make_async_copy(edge, edge, h_s).wait()
    for copies in first + second:
        for copy in copies:
            copy.wait_send()
    for copy in passed + onward:
        copy.wait_send()

    @pl.when(lax.rem(q, 2) == 1)
    def _():
        for copy in relays:
            copy.wait_send()


def per_device(frames, w_in, short_taps, filter_taps, skip_gain, w_out):
    vmem = pl.BlockSpec(memory_space=pltpu.VMEM)
    hbm = pl.BlockSpec(memory_space=pl.ANY)
    dma = pltpu.SemaphoreType.DMA
    row, rowi, tc, ts, cc, cs = tables()
    operands = (
        frames, filter_taps, short_taps, skip_gain.reshape(1, -1), w_in, w_out,
        row, rowi, tc, ts, cc, cs,
    )
    slabs = pltpu.VMEM((ROWS, 8, LANES), BF16)
    scratch = [
        pltpu.VMEM((3, 3, 256), F32), pltpu.VMEM((1, 256), F32),
        pltpu.VMEM((3, 1024, 256), BF16), pltpu.VMEM((2, 512, 256), BF16),
        pltpu.VMEM((256, 128), BF16), pltpu.VMEM((128, 256), BF16),
        pltpu.VMEM((128, 512), F32), pltpu.VMEM((128, 512), F32),
        pltpu.VMEM((512, 512), BF16), pltpu.VMEM((512, 512), BF16),
        pltpu.VMEM((4, HALO + COLS, 256), BF16),
        pltpu.VMEM((512, 256), BF16),
        pltpu.VMEM((HALO + COLS, 768), F32),
        pltpu.VMEM((512, 256), F32), pltpu.VMEM((512, 256), F32),
        pltpu.VMEM((1024, 128), F32),
        slabs, slabs, slabs, slabs, slabs, slabs,
        pltpu.VMEM((2, 512, 128), BF16),
        pltpu.VMEM((2, 512, 512), BF16),
        pltpu.VMEM((128, 512), BF16),
        pltpu.VMEM((256, 512), BF16),
        pltpu.VMEM((2, 256, 512), F32),
        pltpu.VMEM((256, 512), F32), pltpu.VMEM((256, 512), F32),
        pltpu.VMEM((256, 512), BF16),
        pltpu.VMEM((512, 256), F32),
        dma((11,)), dma((8,)),
    ] + [dma((2,))] * 6 + [dma((3,))] * 6 + [dma((6,)), dma((6,)), dma, dma, dma]
    return pl.pallas_call(
        kernel,
        out_shape=jax.ShapeDtypeStruct(frames.shape, BF16),
        in_specs=[hbm] * 12,
        out_specs=vmem,
        scratch_shapes=scratch,
        name="hyena",
        compiler_params=pltpu.CompilerParams(
            collective_id=0, has_side_effects=True, vmem_limit_bytes=30 << 20
        ),
    )(*[pltpu.with_memory_space_constraint(v, pltpu.HBM) for v in operands])


def solution(mesh):
    return jax.shard_map(
        per_device,
        mesh=mesh,
        in_specs=(
            P("tm", "chan"),
            P(None, None, "chan"),
            P(None, None, "chan"),
            P("tm", "chan"),
            P("chan"),
            P(None, "chan"),
        ),
        out_specs=P("tm", "chan"),
        check_vma=False,
    )
```
